32 devices in a mesh: rep: 2 (over x), dp: 16 (over y, z, core).
Axes of the slice: x: 2, y: 2, z: 4, core: 2. Of those that a mesh axis runs over, the one named last changes fastest.
Arguments:
- x: bfloat16 [32, 2048, 896], P(('rep', 'dp')), parts along dimension 0
- dy: bfloat16 [32, 2048, 896], P(('rep', 'dp')), parts along dimension 0
- wq: bfloat16 [2, 896, 896], P(None, 'dp')
- wk: bfloat16 [2, 896, 128], P(None, 'dp')
- wv: bfloat16 [2, 896, 128], P(None, 'dp')
- wo: bfloat16 [2, 896, 896], P(None, 'dp')
- w_gate: bfloat16 [2, 896, 2560], P(None, 'dp')
- w_up: bfloat16 [2, 896, 2560], P(None, 'dp')
- w_down: bfloat16 [2, 2560, 896], P(None, 'dp')
- m_wq: float32 [2, 896, 896], P(None, 'dp')
- m_wk: float32 [2, 896, 128], P(None, 'dp')
- m_wv: float32 [2, 896, 128], P(None, 'dp')
- m_wo: float32 [2, 896, 896], P(None, 'dp')
- m_w_gate: float32 [2, 896, 2560], P(None, 'dp')
- m_w_up: float32 [2, 896, 2560], P(None, 'dp')
- m_w_down: float32 [2, 2560, 896], P(None, 'dp')
- v_wq: float32 [2, 896, 896], P(None, 'dp')
- v_wk: float32 [2, 896, 128], P(None, 'dp')
- v_wv: float32 [2, 896, 128], P(None, 'dp')
- v_wo: float32 [2, 896, 896], P(None, 'dp')
- v_w_gate: float32 [2, 896, 2560], P(None, 'dp')
- v_w_up: float32 [2, 896, 2560], P(None, 'dp')
- v_w_down: float32 [2, 2560, 896], P(None, 'dp')
Outputs:
- output 1: bfloat16 [4, 896, 896], P('rep', 'dp'), parts along dimension 0
- output 2: bfloat16 [4, 896, 128], P('rep', 'dp'), parts along dimension 0
- output 3: bfloat16 [4, 896, 128], P('rep', 'dp'), parts along dimension 0
- output 4: bfloat16 [4, 896, 896], P('rep', 'dp'), parts along dimension 0
- output 5: bfloat16 [4, 896, 2560], P('rep', 'dp'), parts along dimension 0
- output 6: bfloat16 [4, 896, 2560], P('rep', 'dp'), parts along dimension 0
- output 7: bfloat16 [4, 2560, 896], P('rep', 'dp'), parts along dimension 0
- output 8: float32 [4, 896, 896], P('rep', 'dp'), parts along dimension 0
- output 9: float32 [4, 896, 128], P('rep', 'dp'), parts along dimension 0
- output 10: float32 [4, 896, 128], P('rep', 'dp'), parts along dimension 0
- output 11: float32 [4, 896, 896], P('rep', 'dp'), parts along dimension 0
- output 12: float32 [4, 896, 2560], P('rep', 'dp'), parts along dimension 0
- output 13: float32 [4, 896, 2560], P('rep', 'dp'), parts along dimension 0
- output 14: float32 [4, 2560, 896], P('rep', 'dp'), parts along dimension 0
- output 15: float32 [4, 896, 896], P('rep', 'dp'), parts along dimension 0
- output 16: float32 [4, 896, 128], P('rep', 'dp'), parts along dimension 0
- output 17: float32 [4, 896, 128], P('rep', 'dp'), parts along dimension 0
- output 18: float32 [4, 896, 896], P('rep', 'dp'), parts along dimension 0
- output 19: float32 [4, 896, 2560], P('rep', 'dp'), parts along dimension 0
- output 20: float32 [4, 896, 2560], P('rep', 'dp'), parts along dimension 0
- output 21: float32 [4, 2560, 896], P('rep', 'dp'), parts along dimension 0
There are 2 independent parts. The reference program is written for one: setup_inputs(seed, part) draws one part's arguments, and reference() takes and returns one part's arrays. A program takes and returns all parts, laid end to end along the dimension named above; an argument that names none is the same for every part.
All inputs are finite; a program needn't handle non-finite values.
Results may differ from the reference program's by a relative error of at most 0.0358.
Values are sent between devices in bfloat16 or wider.
A program may use at most 2 GiB of HBM per device.

```python
import jax
import jax.numpy as jnp
from jax import lax

SEQUENCES = 16
TOKENS = 2048
D = 896
HEADS = 7
KV_HEADS = 1
HEAD = 128
FF = 2560
LAYERS = 2
THETA = 10000
NAMES = ("wq", "wk", "wv", "wo", "w_gate", "w_up", "w_down")
SHAPES = {
    "wq": (LAYERS, D, HEADS * HEAD),
    "wk": (LAYERS, D, KV_HEADS * HEAD),
    "wv": (LAYERS, D, KV_HEADS * HEAD),
    "wo": (LAYERS, HEADS * HEAD, D),
    "w_gate": (LAYERS, D, FF),
    "w_up": (LAYERS, D, FF),
    "w_down": (LAYERS, FF, D),
}


def bump(key, n, height):
    away = (jnp.arange(n, dtype=jnp.int32) - jax.random.randint(key, (), 0, n, jnp.int32)) % n
    return jnp.where(away < n // 8, height, 1.0)


def together(key, own, strength):
    shared = jax.random.normal(key, own.shape[1:], jnp.float32)
    return (own + strength * shared) * lax.rsqrt(1 + strength * strength)


def setup_inputs(seed: int = 0, part: int = 0) -> dict:
    kx, kdy, ka, kb, kz, kf, kh, kl, *keys = jax.random.split(jax.random.key(seed), 8 + 3 * len(NAMES))
    kx, kdy, ka, kb = (jax.random.fold_in(k, part) for k in (kx, kdy, ka, kb))
    kw, km, kv = (keys[i::3] for i in range(3))
    shape = (SEQUENCES, TOKENS, D)
    much_x, much_dy = jax.random.uniform(kz, (2,), jnp.float32, 0.0, 1.0)
    loud = 2.0 ** jax.random.uniform(jax.random.fold_in(kz, 1), (), jnp.float32, -1.0, 2.0)
    layers = 2.0 ** jax.random.uniform(kl, (LAYERS, 1, 1), jnp.float32, -1.0, 1.0)
    times = {"wq": 1.0, "wk": 1.0, "wv": 2.0, "wo": layers, "w_gate": 1.0, "w_up": bump(kh, FF, 4.0), "w_down": layers}
    x = together(ka, jax.random.normal(kx, shape, jnp.float32), much_x) * bump(kf, D, 4.0)
    dy = together(kb, jax.random.normal(kdy, shape, jnp.float32), much_dy)
    drawn = {"x": x.astype(jnp.bfloat16), "dy": (loud * dy * (SEQUENCES * TOKENS) ** -0.5).astype(jnp.bfloat16)}
    for key, name in zip(kw, NAMES, strict=True):
        drawn[name] = (jax.random.normal(key, SHAPES[name], jnp.float32) * SHAPES[name][1] ** -0.5 * times[name]).astype(jnp.bfloat16)
    for key, name in zip(km, NAMES, strict=True):
        drawn[f"m_{name}"] = 0.1 * jax.random.normal(key, SHAPES[name], jnp.float32)
    for key, name in zip(kv, NAMES, strict=True):
        drawn[f"v_{name}"] = loud * loud * jax.random.uniform(key, SHAPES[name], jnp.float32, 0.2, 0.6)
    return drawn


def matmul(a, w):
    return jnp.dot(a, w, preferred_element_type=jnp.float32).astype(jnp.bfloat16)


def normed(h):
    wide = h.astype(jnp.float32)
    scale = lax.rsqrt(jnp.mean(wide**2, -1, keepdims=True) + 1e-6)
    return (wide * scale).astype(jnp.bfloat16)


def turned(t, theta):
    half = t.shape[-1] // 2
    angle = jnp.arange(t.shape[0], dtype=jnp.float32)[:, None] * theta ** (-jnp.arange(half, dtype=jnp.float32) / half)
    cos, sin = jnp.cos(angle)[:, None], jnp.sin(angle)[:, None]
    a, b = t[..., :half].astype(jnp.float32), t[..., half:].astype(jnp.float32)
    return jnp.concatenate([a * cos - b * sin, b * cos + a * sin], -1).astype(jnp.bfloat16)


def seen_by(q, k, v):
    tokens, kv = q.shape[0], k.shape[1]
    q = q.reshape(tokens, kv, -1, q.shape[-1])
    scores = jnp.einsum("tgsd,ugd->gstu", q.astype(jnp.float32), k.astype(jnp.float32)) * q.shape[-1] ** -0.5
    place = jnp.arange(tokens)
    weights = jax.nn.softmax(jnp.where(place[:, None] >= place, scores, -jnp.inf), -1).astype(jnp.bfloat16)
    return jnp.einsum("gstu,ugd->tgsd", weights.astype(jnp.float32), v.astype(jnp.float32)).astype(jnp.bfloat16).reshape(tokens, -1)


def layer(h, w):
    a = normed(h)
    q, k = (turned(matmul(a, w[name]).reshape(h.shape[0], -1, HEAD), THETA) for name in ("wq", "wk"))
    h = h + matmul(seen_by(q, k, matmul(a, w["wv"]).reshape(h.shape[0], -1, HEAD)), w["wo"])
    b = normed(h)
    gate = jnp.dot(b, w["w_gate"], preferred_element_type=jnp.float32)
    up = jnp.dot(b, w["w_up"], preferred_element_type=jnp.float32)
    return h + matmul((jax.nn.silu(gate) * up).astype(jnp.bfloat16), w["w_down"])


def adamw(w, m, v, g):
    m = 0.9 * m + 0.1 * g
    v = 0.95 * v + 0.05 * g * g
    step = m * lax.rsqrt(v + 1e-8) + 0.1 * w
    return (w - 0.02 * step).astype(jnp.bfloat16), m, v


def stack(weights, h):
    return lax.scan(lambda h, w: (layer(h, w), None), h, weights)[0]


def reference(x, dy, wq, wk, wv, wo, w_gate, w_up, w_down, m_wq, m_wk, m_wv, m_wo, m_w_gate, m_w_up, m_w_down, v_wq, v_wk, v_wv, v_wo, v_w_gate, v_w_up, v_w_down):
    weights = dict(zip(NAMES, (wq, wk, wv, wo, w_gate, w_up, w_down), strict=True))

    def take(so_far, sequence):
        h, by_y = sequence
        _, back = jax.vjp(stack, weights, h)
        by_weights, by_h = back(by_y)
        return jax.tree.map(lambda total, term: total + term.astype(jnp.float32), so_far, by_weights), by_h

    none_yet = {name: jnp.zeros(w.shape, jnp.float32) for name, w in weights.items()}
    by_weights, by_x = lax.scan(take, none_yet, (x, dy))
    gradients = [by_weights[name].astype(jnp.bfloat16).astype(jnp.float32) for name in NAMES]
    first = (m_wq, m_wk, m_wv, m_wo, m_w_gate, m_w_up, m_w_down)
    second = (v_wq, v_wk, v_wv, v_wo, v_w_gate, v_w_up, v_w_down)
    new = [adamw(weights[name].astype(jnp.float32), m, v, g) for name, m, v, g in zip(NAMES, first, second, gradients, strict=True)]
    return tuple(one[which] for which in range(3) for one in new)
```

```python
import functools

import jax
import jax.numpy as jnp
from jax import lax
from jax.experimental import pallas as pl
from jax.experimental.pallas import tpu as pltpu
from jax.sharding import PartitionSpec as P

HEAD = 128
THETA = 10000
NEG = -1e30
HIDDEN = 2 * NEG
LOG2E = 1.4426950408889634
VMEM = 60 * 2**20
BF, F32 = jnp.bfloat16, jnp.float32
ANY = pl.BlockSpec(memory_space=pl.ANY)


def _dot(a, b, ca, cb):
    return lax.dot_general(a, b, (((ca,), (cb,)), ((), ())), preferred_element_type=F32)


def _nn(a, b):
    return _dot(a, b, 1, 0)


def _nt(a, b):
    return _dot(a, b, 1, 1)


def _tn(a, b):
    return _dot(a, b, 0, 0)


def _at():
    return pl.program_id(0)


def _first():
    return _at() == 0


def _whole(*shape):
    return pl.BlockSpec(shape, lambda *_: (0,) * len(shape))


def _rows(tm, n):
    return pl.BlockSpec((tm, n), lambda i, *_: (i, 0))


def _sds(*shape, dtype=BF):
    return jax.ShapeDtypeStruct(shape, dtype)


def _norm(h):
    h = h.astype(F32)
    return h * lax.rsqrt(jnp.mean(h * h, -1, keepdims=True) + 1e-6)


def _norm_bwd(h, d):
    h = h.astype(F32)
    r = lax.rsqrt(jnp.mean(h * h, -1, keepdims=True) + 1e-6)
    return r * d - h * (r * r * r * jnp.mean(d * h, -1, keepdims=True))


def _rot(t, c, s):
    return t * c + pltpu.roll(t, 64, 1) * s


def _unrot(t, c, s):
    return t * c - pltpu.roll(t, 64, 1) * s


MESH = pl.DeviceIdType.MESH


def _flip(n):
    return n + lax.div(n, 4) * (11 - 2 * n)


def _dma(*n):
    return pltpu.SemaphoreType.DMA(n)


class Here:
    def __init__(self):
        self.me = lax.axis_index("dp")
        self.rep = lax.axis_index("rep")
        self.core = lax.rem(self.me, 2)
        self.place = _flip(lax.div(self.me, 2))
        self.next = {"dp": self.device(1, self.core)}
        self.back = {"dp": self.device(7, self.core)}
        self.swap = {"dp": self.device(0, 1 - self.core)}
        self.twin = {"rep": 1 - self.rep}

    def chip(self, n):
        return _flip(lax.rem(self.place + (n + 8), 8))

    def device(self, n, core):
        return 2 * self.chip(n) + core

    def greet(self, twin):
        barrier = pltpu.get_barrier_semaphore()
        to = [self.next, self.back, self.swap] + ([self.twin] if twin else [])
        for d in to:
            pl.semaphore_signal(barrier, inc=1, device_id=d, device_id_type=MESH)
        pl.semaphore_wait(barrier, len(to))


def _remote(src, dst, sems, n, to):
    return pltpu.make_async_remote_copy(src_ref=src, dst_ref=dst, send_sem=sems.at[0, n], recv_sem=sems.at[1, n], device_id=to, device_id_type=MESH)


class Gather:
    twin = True

    def __init__(self, own, layer=None, full=None, first=0, stop=4):
        self.layer, self.first, self.stop = layer, first, stop
        self.ins = list(own) if full is None else [full]
        self.rows, self.n = (own[0].shape[1], sum(w.shape[2] for w in own)) if full is None else (full.shape[0] // 16, full.shape[1])
        self.side = self.n // (3 * HEAD) * HEAD
        self.in_specs = [ANY] * len(self.ins)
        self.outs, self.out_specs = [_sds(16 * self.rows, self.n)], [ANY]
        self.scratch = [_dma(2, 22), _dma(1 + len(self.ins)), pltpu.VMEM((self.rows, self.n) if full is None else (8, HEAD), BF)]
        self.alias = full is not None

    def bind(self, here, ins, outs, scratch):
        (full,), (sems, sem, mine) = outs, scratch
        rows, n, side, core, rep, first, stop = self.rows, self.n, self.side, here.core, here.rep, self.first, self.stop
        wide = n - side
        cols = lambda at, width: pl.ds(pl.multiple_of(at, HEAD), width)
        ring, give, take, every = cols(rep * side, wide), cols(rep * wide, side), cols((1 - rep) * wide, side), slice(None)

        def part(off, who, which):
            return full.at[pl.ds(pl.multiple_of(here.device(off, who) * rows, 8), rows), which]

        def same(off, who, which, n, to):
            return _remote(part(off, who, which), part(off, who, which), sems, n, to)

        def hop(off, n, to):
            return same(off, core, ring, n, to) if off else _remote(mine.at[:, ring], part(off, core, ring), sems, n, to)

        offs = [-1, -2, -3, -4, 1, 2, 3]
        of = lambda k: [k - 1] + ([k + 3] if k < 4 else [])
        hops = [[hop(-k, k, here.next)] + ([hop(k, k + 4, here.back)] if k < 3 else []) for k in range(4)]
        got = [same(o, core, ring, i, here.next) for i, o in enumerate(offs)]
        twin, gotx = ([same(o, core, which, i + 7, here.twin) for i, o in enumerate(offs)] for which in (give, take))
        swap, gots = ([same(o, who, every, i + 14, here.swap) for i, o in enumerate(offs)] for who in (core, 1 - core))
        if not first:
            swap0, got0 = (_remote(mine, part(0, who, every), sems, 21, here.swap) for who in (core, 1 - core))
            keep = pltpu.make_async_copy(mine, part(0, core, every), sem.at[0])
        handed = [k for k in range(1, 5) if first <= k < stop or stop == k == 4]

        def start(*copies):
            for x in copies:
                x.start()

        def hand(k):
            if k in handed:
                start(*(twin[i] for i in of(k)))

        def share(k):
            if k in handed:
                for i in of(k):
                    gotx[i].wait_recv()
                    swap[i].start()

        def begin():
            if first:
                start(*hops[first])
                hand(first)
                return
            at, copies = 0, []
            for i, x in enumerate(ins):
                w = x.shape[2]
                copies.append(pltpu.make_async_copy(x.at[self.layer], mine.at[:, at : at + w], sem.at[i + 1]))
                at += w
            start(*copies)
            for x in copies:
                x.wait()
            start(*hops[0], swap0, keep)

        def tick(k):
            def run():
                for i in of(k):
                    got[i].wait_recv()
                if k < stop:
                    start(*hops[k])
                hand(k)
                share(k - 1)

            return run

        def last():
            blocks = [i for k in handed for i in of(k)]
            for i in blocks:
                gots[i].wait_recv()
            for x in (*(x for h in hops[first:stop] for x in h), *(x[i] for i in blocks for x in (twin, swap))):
                x.wait_send()
            if not first:
                got0.wait_recv()
                swap0.wait_send()
                keep.wait()

        return [begin, *(tick(k) for k in range(first + 1, stop + 1)), *([lambda: share(4)] if stop == 4 else []), last]


class Scatter:
    twin = alias = False

    def __init__(self, mine, theirs, at=0, width=None):
        _, self.rows, n = mine.shape
        self.at, self.n = at, width or n
        buf = lambda k: pltpu.VMEM((k, self.rows, self.n), BF)
        self.ins, self.in_specs = [mine, theirs], [ANY, ANY]
        self.outs = [_sds(8, self.rows, self.n), _sds(self.rows, self.n)]
        self.out_specs = [ANY, _whole(self.rows, self.n)]
        self.scratch = [buf(7), buf(4), buf(4), _dma(2, 15), _dma(4)]

    def bind(self, here, ins, outs, scratch):
        (mine, theirs), (other, g), (came, going, terms, sems, lsem) = ins, outs, scratch
        rows, n = self.rows, self.n
        mine, theirs = (x.at[:, :, pl.ds(self.at, n)] for x in (mine, theirs))
        chunk = max(c for c in range(HEAD, n + 1, HEAD) if n % c == 0 and (c == HEAD or rows * c <= 2**15))
        ahead = [_remote(going.at[k % 2], came.at[k], sems, k, here.next) for k in range(4)]
        back = [_remote(going.at[2 + k % 2], came.at[4 + k], sems, 4 + k, here.back) for k in range(3)]
        order = [4, -3, 3, -2, 2, -1, 1, 0]
        swap = {o: _remote(theirs.at[here.chip(o)], other.at[here.chip(o)], sems, 7 + i, here.swap) for i, o in enumerate(order)}
        fetch = [[4, 3, 2, 1, 0], [-3, -2, -1]]

        def loads(way, k):
            return [pltpu.make_async_copy(src.at[here.chip(fetch[way][k])], terms.at[2 * way + i], lsem.at[2 * way + i]) for i, src in enumerate((mine, other))]

        def load(way, k):
            if k < len(fetch[way]):
                swap[fetch[way][k]].wait_recv()
                for c in loads(way, k):
                    c.start()

        def add(out, way, k, *parts):
            for c in loads(way, k):
                c.wait()

            def body(j, _):
                at = pl.ds(pl.multiple_of(j * chunk, HEAD), chunk)
                out[:, at] = sum(p[:, at].astype(F32) for p in (terms.at[2 * way], terms.at[2 * way + 1], *parts)).astype(BF)
                return 0

            lax.fori_loop(0, n // chunk, body, 0)

        def begin():
            for c in swap.values():
                c.start()

        def swapped():
            load(0, 0)
            load(1, 0)

        def step(k):
            def tick():
                for way, copies in enumerate((ahead, back)):
                    if k < len(copies):
                        if k > 1:
                            copies[k - 2].wait_send()
                        if k:
                            copies[k - 1].wait_recv()
                        add(going.at[2 * way + k % 2], way, k, *([came.at[4 * way + k - 1]] if k else []))
                        copies[k].start()
                        load(way, k + 1)

            return tick

        def end():
            ahead[3].wait_recv()
            back[2].wait_recv()
            add(g, 0, 4, came.at[3], came.at[6])
            for c in (*ahead[2:], *back[1:], *swap.values()):
                c.wait_send()

        return [begin, swapped, *(step(k) for k in range(4)), end]


def _host(body, grid, ins, in_specs, outs, out_specs, scratch, tasks=(), plan=(), cid=None, name=None):
    n_in, n_out, n_scr = len(ins), len(outs), len(scratch)
    t_ins, t_outs, t_scr = ([getattr(t, w) for t in tasks] for w in ("ins", "outs", "scratch"))
    starts = lambda n, xs: [n + sum(map(len, xs[:k])) for k in range(len(xs))]
    alias = {i: o for t, i, o in zip(tasks, starts(n_in, t_ins), starts(n_out, t_outs)) if t.alias}

    def kernel(*refs):
        it = iter(refs)
        take = lambda k: [next(it) for _ in range(k)]
        a, ta = take(n_in), [take(len(x)) for x in t_ins]
        b, tb = take(n_out), [take(len(x)) for x in t_outs]
        c, tc = take(n_scr), [take(len(x)) for x in t_scr]
        todo = []
        if tasks:
            here = Here()
            ticks = [t.bind(here, *x) for t, *x in zip(tasks, ta, tb, tc)]
            todo = sorted(((p, i, fn) for i, (fns, ps) in enumerate(zip(ticks, plan)) for p, fn in zip(ps, fns)), key=lambda x: x[0])

        def hook(n, among=None, first=None):
            if first is not None and tasks:
                @pl.when(first)
                def _():
                    here.greet(any(t.twin for t in tasks))
            for p in dict.fromkeys(p for p, _, _ in todo):
                if among is None or among(p):
                    @pl.when(n == p)
                    def _():
                        for q, _, fn in todo:
                            if q == p:
                                fn()

        body(hook, *a, *b, *c)

    flat = lambda xs: [y for x in xs for y in x]
    got = pl.pallas_call(
        kernel, grid=grid, in_specs=[*in_specs, *flat(t.in_specs for t in tasks)], out_specs=[*out_specs, *flat(t.out_specs for t in tasks)],
        out_shape=[*outs, *flat(t_outs)], scratch_shapes=[*scratch, *flat(t_scr)],
        input_output_aliases=alias,
        compiler_params=pltpu.CompilerParams(vmem_limit_bytes=VMEM, dimension_semantics=("arbitrary",) * len(grid),
                                             **(dict(collective_id=cid, has_side_effects=True) if tasks else {})),
        name=name,
    )(*ins, *flat(t_ins))
    out, at = list(got[:n_out]), n_out
    for x in t_outs:
        at += len(x)
        out.append(got[at - 1])
    return out


def _fill(copies):
    @pl.when(_first())
    def _():
        for c in copies:
            c.start()


def _await(*copies):
    @pl.when(_first())
    def _():
        for c in copies:
            c.wait()


def qkv(h, c, s, w, tm=512, **host):
    t, d = h.shape
    heads, n = d // HEAD, d + 2 * HEAD

    def body(hook, h_ref, c_ref, s_ref, w_ref, a_ref, q_ref, k_ref, v_ref, w_s, sem):
        i = _at()
        copy = pltpu.make_async_copy(w_ref, w_s, sem.at[0])
        _fill([copy])
        hook(i, lambda p: p < t // tm, first=_first())
        a = _norm(h_ref[...]).astype(BF)
        a_ref[...] = a
        _await(copy)
        y = _nn(a, w_s[...]).astype(BF)
        c, s = c_ref[...], s_ref[...]
        for n in range(heads + 1):
            o = _rot(y[:, n * HEAD : (n + 1) * HEAD].astype(F32), c, s).astype(BF)
            if n < heads:
                q_ref[:, n * HEAD : (n + 1) * HEAD] = o
            else:
                k_ref[...] = o
        v_ref[...] = y[:, (heads + 1) * HEAD :]
        hook(i + 1, lambda p: p == t // tm)

    return _host(body, (t // tm,), [h, c, s, w], [_rows(tm, d), _rows(tm, HEAD), _rows(tm, HEAD), ANY],
                 [_sds(t, d), _sds(t, d), _sds(t, HEAD), _sds(t, HEAD)], [_rows(tm, d), _rows(tm, d), _rows(tm, HEAD), _rows(tm, HEAD)],
                 [pltpu.VMEM((d, n), BF), _dma(1)], name="qkv", **host)


def att(q, k, v, bq=512, **host):
    t, d = q.shape
    heads, bk, steps = d // HEAD, bq, t // bq
    scale = HEAD**-0.5
    e = scale * LOG2E
    diagonal = {i * (i + 1) // 2 + i for i in range(steps)}
    last = steps * (steps + 1) // 2

    def body(hook, q_ref, k_ref, v_ref, o_ref, lse_ref, top_s, mix_s):
        iq = _at()
        before = lax.div(iq * (iq + 1), 2)
        hook(-1, lambda p: False, first=_first())
        top_s[...] = jnp.full(top_s.shape, NEG, F32)
        mix_s[...] = jnp.zeros(mix_s.shape, F32)
        ones = jnp.ones((8, bk), BF)

        def block(j, masked):
            hook(before + j, lambda p: p < last and (p in diagonal) == masked)
            here = pl.ds(pl.multiple_of(j * bk, bk), bk)
            kb = k_ref[here, :]
            values = jnp.concatenate([v_ref[here, :].T, ones], axis=0)
            scores = [_nt(kb, q_ref[:, n * HEAD : (n + 1) * HEAD]) for n in range(heads)]
            if masked:
                ok = lax.broadcasted_iota(jnp.int32, (bk, bq), 1) >= lax.broadcasted_iota(jnp.int32, (bk, bq), 0)
            weights, keeps = [], []
            for n, x in enumerate(scores):
                if masked:
                    x = jnp.where(ok, x, HIDDEN)
                old = top_s[n : n + 1, :]
                top = jnp.maximum(old, x.max(axis=0, keepdims=True))
                top_s[n : n + 1, :] = top
                weights.append(jnp.exp2((x - top) * e).astype(BF))
                keeps.append(jnp.exp2((old - top) * e))
            for n, (p, keep) in enumerate(zip(weights, keeps)):
                mix_s[n] = mix_s[n] * keep + _nn(values, p)

        lax.fori_loop(0, iq, lambda j, _: block(j, False), None)
        block(iq, True)
        for n in range(heads):
            total = mix_s[n, HEAD : HEAD + 1, :]
            o_ref[:, n * HEAD : (n + 1) * HEAD] = (mix_s[n, :HEAD, :] * (1 / total)).T.astype(BF)
            lse_ref[n : n + 1, :] = top_s[n : n + 1, :] * scale + jnp.log(total)
        hook(jnp.where(iq == steps - 1, last, -1), lambda p: p == last)

    whole = _whole(t, HEAD)
    return _host(body, (steps,), [q, k, v], [_rows(bq, d), whole, whole], [_sds(t, d), _sds(heads, t, dtype=F32)],
                 [_rows(bq, d), pl.BlockSpec((heads, bq), lambda i: (0, i))],
                 [pltpu.VMEM((heads, bq), F32), pltpu.VMEM((heads, HEAD + 8, bq), F32)], name="att", **host)


def mid(o, h, wo, wg, wu, tm=256, step=512, **host):
    t, d = h.shape
    ff = wg.shape[1]
    parts, steps = ff // step, t // tm

    def body(hook, o_ref, h_ref, wo_ref, wg_ref, wu_ref, h1_ref, b_ref, g_ref, u_ref, act_ref, wo_s, wg_s, wu_s, sem):
        i = _at()
        copies = [pltpu.make_async_copy(a, b, sem.at[n]) for n, (a, b) in enumerate(((wo_ref, wo_s), (wg_ref, wg_s), (wu_ref, wu_s)))]
        _fill(copies)
        hook(-1, lambda p: False, first=_first())
        _await(copies[0])
        y = _nn(o_ref[...], wo_s[...]).astype(BF).astype(F32)
        h1 = (h_ref[...].astype(F32) + y).astype(BF)
        h1_ref[...] = h1
        b = _norm(h1).astype(BF)
        b_ref[...] = b
        _await(*copies[1:])
        for n in range(parts):
            hook(i * parts + n, lambda p: p < parts * steps and p % parts == n)
            at = slice(n * step, (n + 1) * step)
            gate = _nn(b, wg_s[:, at])
            up = _nn(b, wu_s[:, at])
            g_ref[:, at] = gate
            u_ref[:, at] = up
            act_ref[:, at] = (gate * jax.nn.sigmoid(gate) * up).astype(BF)
        hook(i * parts + parts, lambda p: p == parts * steps)

    return _host(body, (steps,), [o, h, wo, wg, wu], [_rows(tm, d), _rows(tm, d), ANY, ANY, ANY],
                 [_sds(t, d), _sds(t, d), _sds(t, ff, dtype=F32), _sds(t, ff, dtype=F32), _sds(t, ff)],
                 [_rows(tm, d), _rows(tm, d), _rows(tm, ff), _rows(tm, ff), _rows(tm, ff)],
                 [pltpu.VMEM((d, d), BF), pltpu.VMEM((d, ff), BF), pltpu.VMEM((d, ff), BF), _dma(3)], name="mid", **host)


def down(act, h1, w, tm=256, **host):
    t, ff = act.shape
    d = h1.shape[1]

    def body(hook, act_ref, h1_ref, w_ref, h_ref, w_s, sem):
        i = _at()
        copy = pltpu.make_async_copy(w_ref, w_s, sem.at[0])
        _fill([copy])
        hook(i, lambda p: p < t // tm, first=_first())
        _await(copy)
        y = _nn(act_ref[...], w_s[...]).astype(BF).astype(F32)
        h_ref[...] = (h1_ref[...].astype(F32) + y).astype(BF)
        hook(i + 1, lambda p: p == t // tm)

    return _host(body, (t // tm,), [act, h1, w], [_rows(tm, ff), _rows(tm, d), ANY], [_sds(t, d)], [_rows(tm, d)],
                 [pltpu.VMEM((ff, d), BF), _dma(1)], name="down", **host)


def mlpb(dh, g, u, h1, wd, wg, wu, wo, tm=256, step=512, **host):
    t, d = dh.shape
    ff = g.shape[1]
    parts, steps = ff // step, t // tm

    def body(hook, dh_ref, g_ref, u_ref, h1_ref, wd_ref, wg_ref, wu_ref, wo_ref, dgu_ref, dh1_ref, do_ref, wd_s, wg_s, wu_s, wo_s, sem):
        i = _at()
        pairs = ((wd_ref, wd_s), (wg_ref, wg_s), (wu_ref, wu_s), (wo_ref, wo_s))
        copies = [pltpu.make_async_copy(a, b, sem.at[n]) for n, (a, b) in enumerate(pairs)]
        _fill(copies)
        hook(-1, lambda p: False, first=_first())
        _await(copies[0])
        dh = dh_ref[...]
        for n in range(parts):
            hook(i * parts + n, lambda p: p < parts * steps and p % parts == n)
            at = slice(n * step, (n + 1) * step)
            da = _nt(dh, wd_s[at, :]).astype(BF).astype(F32)
            gate, up = g_ref[:, at], u_ref[:, at]
            sg = jax.nn.sigmoid(gate)
            dgu_ref[:, at] = (da * up * (sg * (1 + gate * (1 - sg)))).astype(BF)
            dgu_ref[:, ff + n * step : ff + (n + 1) * step] = (da * (gate * sg)).astype(BF)
        _await(*copies[1:])
        db = _nt(dgu_ref[:, :ff], wg_s[...]) + _nt(dgu_ref[:, ff:], wu_s[...])
        dh1 = (dh.astype(F32) + _norm_bwd(h1_ref[...], db.astype(BF).astype(F32))).astype(BF)
        dh1_ref[...] = dh1
        do_ref[...] = _nt(dh1, wo_s[...]).astype(BF)
        hook(i * parts + parts, lambda p: p == parts * steps)

    return _host(body, (steps,), [dh, g, u, h1, wd, wg, wu, wo], [_rows(tm, d), _rows(tm, ff), _rows(tm, ff), _rows(tm, d)] + [ANY] * 4,
                 [_sds(t, 2 * ff), _sds(t, d), _sds(t, d)], [_rows(tm, 2 * ff), _rows(tm, d), _rows(tm, d)],
                 [pltpu.VMEM((ff, d), BF), pltpu.VMEM((d, ff), BF), pltpu.VMEM((d, ff), BF), pltpu.VMEM((d, d), BF), _dma(4)], name="mlpb", **host)


def attb(q, k, v, o, do, lse, c, s, bq=256, bk=256, **host):
    t, d = q.shape
    heads, steps, ratio = d // HEAD, t // bq, bk // bq
    scale = HEAD**-0.5
    e = scale * LOG2E
    blocks = [i // ratio + 1 for i in range(steps)]
    starts = [sum(blocks[:i]) for i in range(steps)]
    last = sum(blocks)
    diagonal = {starts[i] + blocks[i] - 1 for i in range(steps)}

    def body(hook, q_ref, k_ref, v_ref, o_ref, do_ref, lse_ref, c_ref, s_ref, ck_ref, sk_ref, dq_ref, dkv_ref, dq_s, dk_s, dv_s):
        iq = _at()
        whole = lax.div(iq, ratio)
        before = lax.div(ratio * whole * (whole - 1), 2) + (iq - ratio * whole) * whole + iq
        hook(-1, lambda p: False, first=_first())

        @pl.when(_first())
        def _():
            dk_s[...] = jnp.zeros_like(dk_s)
            dv_s[...] = jnp.zeros_like(dv_s)

        dq_s[...] = jnp.zeros_like(dq_s)
        heads_of = [slice(n * HEAD, (n + 1) * HEAD) for n in range(heads)]
        lses = [lse_ref[n : n + 1, :] * LOG2E for n in range(heads)]
        deltas = [(do_ref[:, at].astype(F32) * o_ref[:, at].astype(F32)).T.sum(axis=0, keepdims=True) for at in heads_of]

        def block(j, masked):
            hook(before + j, lambda p: p < last and (p in diagonal) == masked)
            here = pl.ds(pl.multiple_of(j * bk, bk), bk)
            kb, vb = k_ref[here, :], v_ref[here, :]
            kt = kb.T
            scores = [_nt(kb, q_ref[:, at]) for at in heads_of]
            dps = [_nt(vb, do_ref[:, at]) for at in heads_of]
            if masked:
                ok = lax.broadcasted_iota(jnp.int32, (bk, bq), 1) - lax.broadcasted_iota(jnp.int32, (bk, bq), 0) >= j * bk - iq * bq
            for n, at in enumerate(heads_of):
                p = jnp.exp2(scores[n] * e - lses[n])
                if masked:
                    p = jnp.where(ok, p, 0.0)
                ds = (p * (dps[n] - deltas[n])).astype(BF)
                dv_s[here, :] += _nn(p.astype(BF), do_ref[:, at])
                dk_s[here, :] += _nn(ds, q_ref[:, at])
                dq_s[n] += _nn(kt, ds)

        lax.fori_loop(0, whole, lambda j, _: block(j, False), None)
        block(whole, True)
        c, s = c_ref[...], s_ref[...]
        for n, at in enumerate(heads_of):
            dq_ref[:, at] = _unrot((dq_s[n] * scale).T.astype(BF).astype(F32), c, s).astype(BF)

        @pl.when(iq == steps - 1)
        def _():
            dk = (dk_s[...] * scale).astype(BF).astype(F32)
            dkv_ref[:, :HEAD] = _unrot(dk, ck_ref[...], sk_ref[...]).astype(BF)
            dkv_ref[:, HEAD:] = dv_s[...].astype(BF)

        hook(jnp.where(iq == steps - 1, last, -1), lambda p: p == last)

    whole = _whole(t, HEAD)
    return _host(body, (steps,), [q, k, v, o, do, lse, c, s, c, s],
                 [_rows(bq, d), whole, whole, _rows(bq, d), _rows(bq, d), pl.BlockSpec((heads, bq), lambda i: (0, i)), _rows(bq, HEAD), _rows(bq, HEAD), whole, whole],
                 [_sds(t, d), _sds(t, 2 * HEAD)], [_rows(bq, d), _whole(t, 2 * HEAD)],
                 [pltpu.VMEM((heads, HEAD, bq), F32), pltpu.VMEM((t, HEAD), F32), pltpu.VMEM((t, HEAD), F32)], name="attb", **host)


def qkvb(dq, dkv, h, dh1, w, tm=512):
    t, d = h.shape
    n = d + 2 * HEAD

    def body(hook, dq_ref, dkv_ref, h_ref, dh1_ref, w_ref, dh_ref, w_s, sem):
        copy = pltpu.make_async_copy(w_ref, w_s, sem.at[0])
        _fill([copy])
        _await(copy)
        da = _nt(dq_ref[...], w_s[:, :d]) + _nt(dkv_ref[...], w_s[:, d:])
        dh_ref[...] = (dh1_ref[...].astype(F32) + _norm_bwd(h_ref[...], da.astype(BF).astype(F32))).astype(BF)

    return _host(body, (t // tm,), [dq, dkv, h, dh1, w], [_rows(tm, d), _rows(tm, 2 * HEAD), _rows(tm, d), _rows(tm, d), ANY], [_sds(t, d)], [_rows(tm, d)],
                 [pltpu.VMEM((d, n), BF), _dma(1)], name="qkvb")


def _halves(mine_ref, theirs_ref, out, rows):
    me = lax.rem(lax.axis_index("dp"), 2)
    for core in range(2):
        @pl.when(me == core)
        def _():
            for b in range(out.shape[0] // rows):
                ref = mine_ref if b % 2 == core else theirs_ref
                ref[b // 2] = out[b * rows : (b + 1) * rows, :].astype(BF)


def dw_cols(x, g, tn=512, **host):
    t, d = x.shape
    n = g.shape[1]
    rows = d // 16

    def body(hook, x_ref, g_ref, mine_ref, theirs_ref):
        i = _at()
        hook(i, lambda p: p < n // tn, first=_first())
        _halves(mine_ref, theirs_ref, _tn(x_ref[...], g_ref[...]), rows)
        hook(i + 1, lambda p: p == n // tn)

    spec = pl.BlockSpec((8, rows, tn), lambda j: (0, 0, j))
    return _host(body, (n // tn,), [x, g], [_whole(t, d), pl.BlockSpec((t, tn), lambda j: (0, j))],
                 [_sds(8, rows, n)] * 2, [spec, spec], [], name="dw_cols", **host)


def dw_rows(x, g, chips=2, **host):
    t, d = x.shape
    n = g.shape[1]
    rows = d // 16

    def body(hook, x_ref, g_ref, mine_ref, theirs_ref):
        i = _at()
        hook(i, lambda p: p < 8 // chips, first=_first())
        _halves(mine_ref, theirs_ref, _tn(x_ref[...], g_ref[...]), rows)
        hook(i + 1, lambda p: p == 8 // chips)

    spec = pl.BlockSpec((chips, rows, n), lambda j: (j, 0, 0))
    return _host(body, (8 // chips,), [x, g], [pl.BlockSpec((t, 2 * chips * rows), lambda j: (0, j)), _whole(t, n)],
                 [_sds(8, rows, n)] * 2, [spec, spec], [], name="dw_rows", **host)


def dw_tokens(x, gs, tk=1024, **host):
    t, d = x.shape
    n = sum(g.shape[1] for g in gs)
    rows, steps = d // 16, t // tk

    def body(hook, x_ref, *rest):
        g_refs, (mine_ref, theirs_ref, acc) = rest[: len(gs)], rest[len(gs) :]
        i = _at()
        hook(i, lambda p: p < steps, first=_first())
        at = 0
        for g_ref in g_refs:
            cols = slice(at, at + g_ref.shape[1])
            add = _tn(x_ref[...], g_ref[...])

            @pl.when(_first())
            def _():
                acc[:, cols] = add

            @pl.when(i > 0)
            def _():
                acc[:, cols] += add

            at += g_ref.shape[1]

        @pl.when(i == steps - 1)
        def _():
            _halves(mine_ref, theirs_ref, acc, rows)

        hook(i + 1, lambda p: p == steps)

    spec = _whole(8, rows, n)
    return _host(body, (steps,), [x, *gs], [_rows(tk, d)] + [_rows(tk, g.shape[1]) for g in gs], [_sds(8, rows, n)] * 2, [spec, spec],
                 [pltpu.VMEM((d, n), F32)], name="dw_tokens", **host)


def begin(t, **host):
    half = HEAD // 2

    def body(hook, f_ref, c_ref, s_ref):
        hook(0, lambda p: p == 0, first=_first())

        def rows(j, _):
            at = pl.ds(pl.multiple_of(j * HEAD, HEAD), HEAD)
            angle = (lax.broadcasted_iota(jnp.int32, (HEAD, HEAD), 0) + j * HEAD).astype(F32) * f_ref[...]
            sin = jnp.sin(angle)
            c_ref[at, :] = jnp.cos(angle)
            s_ref[at, :] = jnp.where(lax.broadcasted_iota(jnp.int32, (HEAD, HEAD), 1) < half, -sin, sin)
            return 0

        lax.fori_loop(0, t // HEAD, rows, 0)
        for n in range(1, 1 + max(map(max, host["plan"]))):
            hook(n, lambda p: p == n)

    one = -jnp.arange(half, dtype=F32) / half
    f = THETA ** jnp.concatenate([one, one])[None]
    whole = lambda r: _whole(r, HEAD)
    return _host(body, (1,), [f], [whole(1)], [_sds(t, HEAD, dtype=F32)] * 2, [whole(t)] * 2, [], name="begin", **host)


def adamw(w, m, v, g):
    m = 0.9 * m + 0.1 * g
    v = 0.95 * v + 0.05 * g * g
    step = m * lax.rsqrt(v + 1e-8) + 0.1 * w
    return (w - 0.02 * step).astype(BF), m, v


def alone(count, **host):
    def body(hook):
        for n in range(count):
            hook(n, lambda p: p == n, first=None if n else _first())

    return _host(body, (1,), [], [], [], [], [], name="alone", **host)


def steps(begin, swapped, first, gap, end):
    return [begin, swapped, *(int(first + gap * k) for k in range(4)), end]


def solution(mesh):
    def step(x, dy, *arrays):
        weights, m, v = (arrays[i : i + 7] for i in (0, 7, 14))
        wq, wk, wv, wo, wg, wu, wd = weights
        d = wq.shape[2]
        cids = iter(range(1, 99))

        def tasks(*pairs):
            return dict(tasks=[t for t, _ in pairs], plan=[p for _, p in pairs], cid=next(cids))

        def more(part, first, stop, *plans):
            return tasks(*((Gather((), full=f, first=first, stop=stop), p) for f, p in zip(part, plans)))

        def early(layer, *plans):
            return [(Gather((w,), layer, stop=1), p) for w, p in zip((wo, wg, wu), plans)]

        second, third = [(0, 4, 4)] * 3, ((0, 5, 9, 10, 10), (0, 3, 7, 9, 10), (0, 5, 9, 10, 10))
        slow = (*range(0, 40, 8), 39, 40)

        (h0,), (dh,) = x, dy
        c, s, fqkv0, *part = begin(x.shape[1], **tasks((Gather((wq, wk, wv), 0), range(7)), *early(0, (0, 1, 5), (1, 2, 5), (2, 3, 5))))
        a0, q0, k0, v0, *part = qkv(h0, c, s, fqkv0, **more(part, 1, 2, *second))
        o0, lse0, fo0, fg0, fu0 = att(q0, k0, v0, **more(part, 2, 4, *third))
        h1_0, b0, g0, u0, act0, fd0, fqkv1 = mid(o0, h0, fo0, fg0, fu0, **tasks(
            (Gather((wd,), 0), slow), (Gather((wq, wk, wv), 1), (*range(4, 36, 8), 35, 38, 40))))
        h_1, *part = down(act0, h1_0, fd0, **tasks(*early(1, *[(0, 7, 8)] * 3)))
        a1, q1, k1, v1, *part = qkv(h_1, c, s, fqkv1, **more(part, 1, 2, *second))
        o1, lse1, fo1, fg1, fu1 = att(q1, k1, v1, **more(part, 2, 4, *third))
        h1_1, b1, g1, u1, act1, fd1 = mid(o1, h_1, fo1, fg1, fu1, **tasks((Gather((wd,), 1), slow)))

        def halves(pair):
            n = pair[0].shape[2] // 2
            return [(Scatter(*pair, at, n), p) for at, p in ((0, steps(0, 1, 2, 7.5, 33)), (n, steps(0, 2, 3, 9, 36)))]

        pd1 = dw_rows(act1, dh)
        dgu1, dh1_1, do1, gd1 = mlpb(dh, g1, u1, h1_1, fd1, fg1, fu1, fo1, **tasks((Scatter(*pd1), steps(0, 2, 5, 7.5, 35))))
        pgu1 = dw_cols(b1, dgu1)
        po1 = dw_tokens(o1, [dh1_1])
        dq1, dkv1, gg1, gu1 = attb(q1, k1, v1, o1, do1, lse1, c, s, **tasks(*halves(pgu1)))
        pqkv1 = dw_tokens(a1, [dq1, dkv1], 2048)
        (dh,) = qkvb(dq1, dkv1, h_1, dh1_1, fqkv1)
        pd0 = dw_rows(act0, dh)
        late = steps(0, 5, 7, 8.5, 40)
        dgu0, dh1_0, do0, gd0, go1, gqkv1 = mlpb(dh, g0, u0, h1_0, fd0, fg0, fu0, fo0, **tasks(
            (Scatter(*pd0), steps(0, 2, 5, 8.4, 37)), (Scatter(*po1), late), (Scatter(*pqkv1), late)))
        po0 = dw_tokens(o0, [dh1_0])
        *pgu0, go0 = dw_cols(b0, dgu0, **tasks((Scatter(*po0), steps(0, 1, 2, 2, 10))))
        dq0, dkv0, gg0, gu0 = attb(q0, k0, v0, o0, do0, lse0, c, s, **tasks(*halves(pgu0)))
        pqkv0 = dw_tokens(a0, [dq0, dkv0], 2048)
        (gqkv0,) = alone(7, **tasks((Scatter(*pqkv0), range(7))))
        split = lambda g: jnp.split(g, (d, d + HEAD), 1)
        gradients = zip((*split(gqkv0), go0, gg0, gu0, gd0), (*split(gqkv1), go1, gg1, gu1, gd1))
        new = [adamw(w.astype(F32), m, v, jnp.stack(g).astype(F32)) for w, m, v, g in zip(weights, m, v, gradients, strict=True)]
        return tuple(one[which] for which in range(3) for one in new)

    states, cut = P(("rep", "dp"), None, None), P(None, "dp", None)
    return jax.shard_map(step, mesh=mesh, in_specs=(states, states) + (cut,) * 21, out_specs=(P("rep", "dp", None),) * 21, check_vma=False)
```
